32 devices in a mesh: row: 8 (over y, x, core), col: 4 (over z).
Axes of the slice: x: 2, y: 2, z: 4, core: 2. Of those that a mesh axis runs over, the one named last changes fastest.
Arguments:
- tensor: float32 [128, 128, 768], P('row', 'col'), may hold values from -6 to 6
- start_one: float32 [128, 64], P('row'), may hold values from -0.5 to 0.5
- start_two: float32 [128, 64], P('col'), may hold values from -0.5 to 0.5
- start_three: float32 [768, 64], replicated, may hold values from -0.21875 to 0.21875
Outputs:
- factor_one: float32 [128, 64], replicated
- factor_two: float32 [128, 64], replicated
- factor_three: float32 [768, 64], replicated
- core: float32 [64, 64, 64], P(None, 'row', 'col')
The draws below stay inside these ranges and needn't reach their ends.
All inputs are finite; a program needn't handle non-finite values.
Results may differ from the reference program's by a relative error of at most 0.0003.
Values sent between devices are 32-bit elements; how exact they have to be, the bound alone decides.
No kernel may reach another device: no remote copies, remote signals or barrier semaphores. Data moves between devices by JAX's collectives and lax.ppermute only.
A program may use at most 64 MiB of HBM per device.

```python
import math
import jax
import jax.numpy as jnp
from jax import lax

N3 = 768
RANK = 64
STEPS = 4
N1 = 128
N2 = 128


def levels(key, extent, cuts, least, top_value):
    def one(position, parts):
        steps = jax.random.uniform(jax.random.fold_in(jax.random.fold_in(key, 6), position), (parts,), jnp.float32, least / len(cuts), top_value / len(cuts))
        return jnp.repeat(jnp.exp(steps), extent[position] // parts).reshape((-1,) + (1,) * (len(extent) - position - 1))

    gain = one(*cuts[0])
    for cut in cuts[1:]:
        gain = gain * one(*cut)
    return gain


def centred(own_key, extent, scale, reach, shards=(), held_as=jnp.bfloat16):
    gain = levels(own_key, extent, shards, -0.22, 0.18) if shards else 1.0
    array = jax.random.normal(own_key, extent, jnp.float32) * scale * gain
    return jnp.minimum(jnp.maximum(array, -reach), reach).astype(held_as)


def setup_inputs(seed: int = 0) -> dict:
    seeds = jax.random.split(jax.random.key(seed), 5)
    return {
        "tensor": centred(seeds[0], (N1, N2, N3), 1.0, 6.0, ((0, 8), (1, 4)), jnp.float32),
        "start_one": centred(seeds[1], (N1, RANK), N1 ** -0.5, 0.5, ((0, 8),), jnp.float32),
        "start_two": centred(seeds[2], (N2, RANK), N2 ** -0.5, 0.5, ((0, 4),), jnp.float32),
        "start_three": centred(seeds[3], (N3, RANK), N3 ** -0.5, 0.21875, (), jnp.float32),
    }


HIGHEST = lax.Precision.HIGHEST

def orthonormal(matrix):
    inner = jnp.dot(matrix.T.astype(jnp.float32), matrix.astype(jnp.float32), precision=HIGHEST, preferred_element_type=jnp.float32)
    lower = jnp.linalg.cholesky(inner)
    return jax.scipy.linalg.solve_triangular(lower, matrix.T, lower=True).T

def iterate(gram, start):
    basis = start
    for iteration in range(STEPS):
        basis = orthonormal(jnp.dot(gram.astype(jnp.float32), basis.astype(jnp.float32), precision=HIGHEST, preferred_element_type=jnp.float32))
    return basis

def self_gram(slab):
    return jnp.dot(slab.astype(jnp.float32), slab.T.astype(jnp.float32), precision=HIGHEST, preferred_element_type=jnp.float32)

def reference(tensor, start_one, start_two, start_three):
    contracted = jnp.einsum('ijk,kc->ijc', tensor, start_three, precision=HIGHEST)
    slab_one = jnp.einsum('ijc,jb->ibc', contracted, start_two, precision=HIGHEST).reshape(N1, RANK * RANK)
    basis_one = iterate(self_gram(slab_one), start_one)
    slab_two = jnp.einsum('ijc,ia->jac', contracted, basis_one, precision=HIGHEST).reshape(N2, RANK * RANK)
    basis_two = iterate(self_gram(slab_two), start_two)
    partial_three = jnp.einsum('ijk,ia->ajk', tensor, basis_one, precision=HIGHEST)
    slab_three = jnp.einsum('ajk,jb->kab', partial_three, basis_two, precision=HIGHEST).reshape(N3, RANK * RANK)
    basis_three = iterate(self_gram(slab_three), start_three)
    core = jnp.dot(basis_three.T.astype(jnp.float32), slab_three.astype(jnp.float32), precision=HIGHEST, preferred_element_type=jnp.float32).reshape(RANK, RANK, RANK)
    factor_one = basis_one * math.sqrt(N1)
    factor_two = basis_two * math.sqrt(N2)
    factor_three = basis_three * math.sqrt(N3)
    return (factor_one, factor_two, factor_three, core)
```

```python
import math

import jax
import jax.numpy as jnp
from jax import lax
from jax.experimental import pallas as pl
from jax.experimental.pallas import tpu as pltpu
from jax.sharding import PartitionSpec as P

STEPS = 4
PANEL = 8
BLOCK = 128
WIDE = 256
AXES = ("row", "col")

HIGHEST = lax.Precision.HIGHEST


def product(left, right):
    return jnp.dot(left, right, precision=HIGHEST, preferred_element_type=jnp.float32)


def left_product(left, right):
    return lax.dot_general(
        left, right, (((0,), (0,)), ((), ())), precision=HIGHEST, preferred_element_type=jnp.float32
    )


def right_product(left, right):
    return lax.dot_general(
        left, right, (((1,), (1,)), ((), ())), precision=HIGHEST, preferred_element_type=jnp.float32
    )


def cross_product(left, right):
    return lax.dot_general(
        left, right, (((0,), (1,)), ((), ())), precision=HIGHEST, preferred_element_type=jnp.float32
    )


def orthonormal(matrix, inner):
    lower = jnp.linalg.cholesky(inner)
    return jax.scipy.linalg.solve_triangular(lower, matrix.T, lower=True).T


def pairing(local, block_rows):
    return right_product(local, block_rows)


def spread(row, like):
    return jnp.broadcast_to(row, like.shape)


def lower_inverse(inner):
    size = inner.shape[0]
    eye = (
        lax.broadcasted_iota(jnp.int32, (size, size), 0) == lax.broadcasted_iota(jnp.int32, (size, size), 1)
    ).astype(jnp.float32)
    whole = jnp.concatenate([inner, eye], axis=1)
    panels = size // PANEL
    work = [whole[p * PANEL : (p + 1) * PANEL] for p in range(panels)]
    sub = lax.broadcasted_iota(jnp.int32, work[0].shape, 0)
    out = []
    for p in range(panels):
        cols = {
            i: [spread(work[i][:, p * PANEL + k : p * PANEL + k + 1], work[i]) for k in range(PANEL)]
            for i in range(p, panels)
        }
        scale = jnp.zeros_like(work[p])
        for k in range(PANEL):
            row = spread(work[p][k : k + 1], work[p])
            pivot = spread(cols[p][k][k : k + 1], work[p])
            scale = jnp.where(sub == k, lax.rsqrt(pivot), scale)
            recip = 1.0 / pivot
            across = [spread(cols[p][m][k : k + 1], work[p]) * recip for m in range(k + 1, PANEL)]
            row = row * recip
            for i in range(p, panels):
                factor = cols[i][k]
                if i == p:
                    factor = jnp.where(sub > k, factor, 0.0)
                work[i] = work[i] - factor * row
                for m in range(k + 1, PANEL):
                    cols[i][m] = cols[i][m] - factor * across[m - k - 1]
        out.append((work[p] * scale)[:, size:])
    return jnp.concatenate(out, axis=0)


def settle_kernel(gram_ref, start_ref, out_ref):
    out_ref[...] = iterate(gram_ref[...], start_ref[...])


def settle(gram_whole, basis):
    return call(settle_kernel, "settle", [basis.shape], gram_whole, basis)[0]


def general(tensor, start_one, start_two, start_three):
    rows_one, rows_two, depth = tensor.shape
    rank = start_three.shape[1]
    flat = tensor.reshape(rows_one * rows_two, depth)
    contracted = cross_product(start_three, flat).reshape(rank, rows_one, rows_two)
    part_one = jnp.einsum("cij,jb->ibc", contracted, start_two, precision=HIGHEST).reshape(
        rows_one, rank * rank
    )
    slab_one = lax.psum_scatter(part_one, "col", scatter_dimension=1, tiled=True)
    slab_rows_one = lax.all_gather(slab_one, "row", axis=0, tiled=True)
    gram_one = lax.psum(right_product(slab_rows_one, slab_rows_one), "col")
    basis_one = settle(gram_one, lax.all_gather(start_one, "row", axis=0, tiled=True))
    own_one = lax.dynamic_slice_in_dim(basis_one, lax.axis_index("row") * rows_one, rows_one, 0)
    part_two = jnp.einsum("cij,ia->jac", contracted, own_one, precision=HIGHEST).reshape(
        rows_two, rank * rank
    )
    slab_two = lax.psum_scatter(part_two, "row", scatter_dimension=1, tiled=True)
    slab_rows_two = lax.all_gather(slab_two, "col", axis=0, tiled=True)
    gram_two = lax.psum(right_product(slab_rows_two, slab_rows_two), "row")
    basis_two = settle(gram_two, lax.all_gather(start_two, "col", axis=0, tiled=True))
    own_two = lax.dynamic_slice_in_dim(basis_two, lax.axis_index("col") * rows_two, rows_two, 0)
    received = lax.all_to_all(tensor, "row", split_axis=2, concat_axis=0, tiled=True)
    count, items, cells = received.shape
    merged = left_product(basis_one, received.reshape(count, items * cells))
    mixed = merged.reshape(rank, items, cells)
    part_three = jnp.einsum("ajk,jb->kba", mixed, own_two, precision=HIGHEST)
    cells_here = part_three.shape[0]
    slab_three = lax.psum_scatter(
        part_three.reshape(cells_here, rank * rank), "col", scatter_dimension=1, tiled=True
    )
    gram_part_three = pairing(slab_three, lax.all_gather(slab_three, "row", axis=0, tiled=True))
    gram_three = lax.psum(gram_part_three, "col")
    basis_three = start_three
    own_three = start_three
    for iteration in range(STEPS):
        image = product(gram_three, basis_three)
        inner = lax.psum(left_product(image, image), "row")
        own_three = orthonormal(image, inner)
        basis_three = lax.all_gather(own_three, "row", axis=0, tiled=True)
    core_part = left_product(own_three, slab_three)
    core_part = core_part.reshape(rank, core_part.shape[1] // rank, rank)
    core = lax.psum_scatter(core_part, "row", scatter_dimension=2, tiled=True).transpose(0, 2, 1)
    factor_one = basis_one * math.sqrt(basis_one.shape[0])
    factor_two = basis_two * math.sqrt(basis_two.shape[0])
    factor_three = basis_three * math.sqrt(basis_three.shape[0])
    return (factor_one, factor_two, factor_three, core)


VMEM = pl.BlockSpec(memory_space=pltpu.VMEM)


def call(kernel, name, outs, *args):
    return pl.pallas_call(
        kernel,
        out_shape=[jax.ShapeDtypeStruct(shape, jnp.float32) for shape in outs],
        in_specs=[VMEM] * len(args),
        out_specs=[VMEM] * len(outs),
        name=name,
    )(*args)


def iterate(gram, start):
    size = start.shape[0]
    extra = -size % WIDE
    gram = jnp.pad(gram, ((0, extra), (0, extra)))

    def step(_, turned):
        image = product(turned, gram)
        return product(lower_inverse(right_product(image, image)), image)

    return lax.fori_loop(0, STEPS, step, jnp.pad(start.T, ((0, 0), (0, extra))))[:, :size].T


def gram_of(slabs):
    total = right_product(slabs[0], slabs[0])
    for slab in slabs[1:]:
        total = total + right_product(slab, slab)
    return total


def open_kernel(cont_ref, start_ref, gram_ref):
    slabs = [product(cont_ref[c], start_ref[...]) for c in range(cont_ref.shape[0])]
    gram_ref[...] = gram_of(slabs)


def first_kernel(gram_ref, start_ref, cont_ref, basis_ref, factor_ref, next_ref):
    basis = iterate(gram_ref[...], start_ref[...])
    basis_ref[...] = basis
    factor_ref[...] = basis * math.sqrt(basis.shape[0])
    slabs = [left_product(cont_ref[c], basis) for c in range(cont_ref.shape[0])]
    next_ref[...] = gram_of(slabs)


def second_kernel(gram_ref, start_ref, factor_ref):
    basis = iterate(gram_ref[...], start_ref[...])
    factor_ref[...] = basis


def slab_kernel(left_ref, right_ref, tensor_ref, factor_ref, slab_ref):
    right = right_ref[...]
    factor_ref[...] = right * math.sqrt(right.shape[0])
    count, rows, cols = tensor_ref.shape
    half = product(tensor_ref[...].reshape(count * rows, cols), right)
    for k in range(count):
        slab_ref[k] = left_product(left_ref[...], half[k * rows : (k + 1) * rows])


def pairs(blocks):
    return [(i, j) for i in range(blocks) for j in range(i, blocks)]


def pair_kernel(slab_ref, gram_ref):
    for n, (i, j) in enumerate(pairs(slab_ref.shape[0] // BLOCK)):
        gram_ref[n * BLOCK : (n + 1) * BLOCK] = right_product(
            slab_ref[i * BLOCK : (i + 1) * BLOCK], slab_ref[j * BLOCK : (j + 1) * BLOCK]
        )


def third_kernel(packed_ref, start_ref, slab_ref, factor_ref, core_ref, gram_ref):
    for n, (i, j) in enumerate(pairs(slab_ref.shape[0] // BLOCK)):
        block = packed_ref[n * BLOCK : (n + 1) * BLOCK]
        gram_ref[i * BLOCK : (i + 1) * BLOCK, j * BLOCK : (j + 1) * BLOCK] = block
        if i != j:
            gram_ref[j * BLOCK : (j + 1) * BLOCK, i * BLOCK : (i + 1) * BLOCK] = block.T
    basis = iterate(gram_ref[...], start_ref[...])
    factor_ref[...] = basis * math.sqrt(basis.shape[0])
    core_ref[...] = left_product(basis, slab_ref[...])


def swap(x, axis, mask):
    count = lax.axis_size(axis)
    return lax.ppermute(x, axis, [(i, i ^ mask) for i in range(count)])


def tree(parts):
    while len(parts) > 1:
        parts = [parts[i] + parts[i + 1] for i in range(0, len(parts), 2)]
    return parts[0]


def sum_small(x):
    x = x + swap(x, "row", 1)
    x = tree([x] + [swap(x, "row", m) for m in range(2, lax.axis_size("row"), 2)])
    return tree([x] + [swap(x, "col", m) for m in range(1, lax.axis_size("col"))])


def bit(axis, mask):
    return (lax.axis_index(axis) & mask) != 0


def halve(x, axis, mask):
    rows = x.shape[0] // 2
    low, high = x[:rows], x[rows:]
    upper = bit(axis, mask)
    return jnp.where(upper, high, low) + swap(jnp.where(upper, low, high), axis, mask)


def double(x, axis, mask):
    other = swap(x, axis, mask)
    upper = bit(axis, mask)
    return jnp.concatenate([jnp.where(upper, other, x), jnp.where(upper, x, other)], axis=0)


def spread_rows(x, axis):
    mask = 1
    while mask < lax.axis_size(axis):
        x = double(x, axis, mask)
        mask *= 2
    return x


def sum_large(x):
    x = halve(x, "row", 1)
    rows = x.shape[0] // 2
    masks = [m for m in (2, 4, 8, 16) if m < lax.axis_size("row")]
    lanes = [(x[:rows], masks), (x[rows:], masks[::-1])]
    done = []
    for part, order in lanes:
        for mask in order:
            part = halve(part, "row", mask)
        mask = 1
        while mask < lax.axis_size("col"):
            part = part + swap(part, "col", mask)
            mask *= 2
        for mask in order[::-1]:
            part = double(part, "row", mask)
        done.append(part)
    return double(jnp.concatenate(done, axis=0), "row", 1)


def swift(tensor, start_one, start_two, start_three):
    rows_one, rows_two, depth = tensor.shape
    rank = start_three.shape[1]
    ways_one, ways_two = lax.axis_size("row"), lax.axis_size("col")
    ways = ways_one * ways_two
    full_one, full_two = rows_one * ways_one, rows_two * ways_two
    flat = tensor.reshape(rows_one * rows_two, depth)
    two = spread_rows(start_two, "col")
    one = spread_rows(start_one, "row")

    def regroup(x):
        count = x.shape[0] // ways
        x = lax.all_to_all(x.reshape(ways, count, rows_one * rows_two), AXES, 0, 0, tiled=True)
        x = x.reshape(ways_one, ways_two, count, rows_one, rows_two)
        return x.transpose(2, 0, 3, 1, 4).reshape(count, full_one, full_two)

    contracted = regroup(cross_product(start_three, flat))
    cells = regroup(flat.T)
    (gram,) = call(open_kernel, "open", [(full_one, full_one)], contracted, two)
    basis_one, factor_one, gram = call(
        first_kernel,
        "first",
        [(full_one, rank), (full_one, rank), (full_two, full_two)],
        sum_small(gram),
        one,
        contracted,
    )
    (basis_two,) = call(second_kernel, "second", [(full_two, rank)], sum_small(gram), two)
    count = depth // ways
    factor_two, slab = call(
        slab_kernel, "slab", [(full_two, rank), (count, rank, rank)], basis_one, basis_two, cells
    )
    own_a, own_b = rank // ways_one, rank // ways_two
    slab = slab.reshape(count, ways_one, own_a, ways_two, own_b).transpose(1, 3, 0, 2, 4)
    slab = lax.all_to_all(slab.reshape(ways, count, own_a * own_b), AXES, 0, 0, tiled=True)
    slab = slab.reshape(depth, own_a * own_b)
    blocks = len(pairs(depth // BLOCK))
    (packed,) = call(pair_kernel, "pair", [(blocks * BLOCK, BLOCK)], slab)
    factor_three, core = pl.pallas_call(
        third_kernel,
        out_shape=[
            jax.ShapeDtypeStruct((depth, rank), jnp.float32),
            jax.ShapeDtypeStruct((rank, own_a * own_b), jnp.float32),
        ],
        in_specs=[VMEM] * 3,
        out_specs=[VMEM] * 2,
        scratch_shapes=[pltpu.VMEM((depth, depth), jnp.float32)],
        name="third",
    )(sum_large(packed), start_three, slab)
    return (factor_one, factor_two, factor_three, core.reshape(rank, own_a, own_b))


def power_of_two(value):
    return value & (value - 1) == 0


def on_device(tensor, start_one, start_two, start_three):
    rank, depth = start_three.shape[1], start_three.shape[0]
    ways_one, ways_two = lax.axis_size("row"), lax.axis_size("col")
    ways = ways_one * ways_two
    even = power_of_two(ways_one) and power_of_two(ways_two) and ways_one > 1
    blocks = len(pairs(depth // BLOCK)) * BLOCK
    even = even and rank % ways == 0 and depth % ways == 0 and depth % BLOCK == 0
    if even and blocks % (8 * 2 * ways_one) == 0:
        return swift(tensor, start_one, start_two, start_three)
    return general(tensor, start_one, start_two, start_three)


def solution(mesh):
    return jax.shard_map(
        on_device,
        mesh=mesh,
        in_specs=(P("row", "col", None), P("row", None), P("col", None), P()),
        out_specs=(P(), P(), P(), P(None, "row", "col")),
        check_vma=False,
    )
```

```python
import functools
import math

import jax
import jax.numpy as jnp
from jax import lax
from jax.experimental import pallas as pl
from jax.experimental.pallas import tpu as pltpu
from jax.sharding import PartitionSpec as P

STEPS = 4
PANEL = 8
BLOCK = 128
WIDE = 256
AXES = ("row", "col")

HIGHEST = lax.Precision.HIGHEST


def product(left, right):
    return jnp.dot(left, right, precision=HIGHEST, preferred_element_type=jnp.float32)


def left_product(left, right):
    return lax.dot_general(
        left, right, (((0,), (0,)), ((), ())), precision=HIGHEST, preferred_element_type=jnp.float32
    )


def right_product(left, right):
    return lax.dot_general(
        left, right, (((1,), (1,)), ((), ())), precision=HIGHEST, preferred_element_type=jnp.float32
    )


def cross_product(left, right):
    return lax.dot_general(
        left, right, (((0,), (1,)), ((), ())), precision=HIGHEST, preferred_element_type=jnp.float32
    )


def orthonormal(matrix, inner):
    lower = jnp.linalg.cholesky(inner)
    return jax.scipy.linalg.solve_triangular(lower, matrix.T, lower=True).T


def pairing(local, block_rows):
    return right_product(local, block_rows)


def spread(row, like):
    return jnp.broadcast_to(row, like.shape)


def lower_inverse(inner):
    size = inner.shape[0]
    eye = (
        lax.broadcasted_iota(jnp.int32, (size, size), 0) == lax.broadcasted_iota(jnp.int32, (size, size), 1)
    ).astype(jnp.float32)
    whole = jnp.concatenate([inner, eye], axis=1)
    panels = size // PANEL
    work = [whole[p * PANEL : (p + 1) * PANEL] for p in range(panels)]
    sub = lax.broadcasted_iota(jnp.int32, work[0].shape, 0)
    out = []
    for p in range(panels):
        cols = {
            i: [spread(work[i][:, p * PANEL + k : p * PANEL + k + 1], work[i]) for k in range(PANEL)]
            for i in range(p, panels)
        }
        scale = jnp.zeros_like(work[p])
        for k in range(PANEL):
            row = spread(work[p][k : k + 1], work[p])
            pivot = spread(cols[p][k][k : k + 1], work[p])
            scale = jnp.where(sub == k, lax.rsqrt(pivot), scale)
            recip = 1.0 / pivot
            across = [spread(cols[p][m][k : k + 1], work[p]) * recip for m in range(k + 1, PANEL)]
            row = row * recip
            for i in range(p, panels):
                factor = cols[i][k]
                if i == p:
                    factor = jnp.where(sub > k, factor, 0.0)
                work[i] = work[i] - factor * row
                for m in range(k + 1, PANEL):
                    cols[i][m] = cols[i][m] - factor * across[m - k - 1]
        out.append((work[p] * scale)[:, size:])
    return jnp.concatenate(out, axis=0)


def settle_kernel(gram_ref, start_ref, out_ref):
    out_ref[...] = iterate(gram_ref[...], start_ref[...])


def settle(gram_whole, basis):
    return call(settle_kernel, "settle", [basis.shape], gram_whole, basis)[0]


def general(tensor, start_one, start_two, start_three):
    rows_one, rows_two, depth = tensor.shape
    rank = start_three.shape[1]
    flat = tensor.reshape(rows_one * rows_two, depth)
    contracted = cross_product(start_three, flat).reshape(rank, rows_one, rows_two)
    part_one = jnp.einsum("cij,jb->ibc", contracted, start_two, precision=HIGHEST).reshape(
        rows_one, rank * rank
    )
    slab_one = lax.psum_scatter(part_one, "col", scatter_dimension=1, tiled=True)
    slab_rows_one = lax.all_gather(slab_one, "row", axis=0, tiled=True)
    gram_one = lax.psum(right_product(slab_rows_one, slab_rows_one), "col")
    basis_one = settle(gram_one, lax.all_gather(start_one, "row", axis=0, tiled=True))
    own_one = lax.dynamic_slice_in_dim(basis_one, lax.axis_index("row") * rows_one, rows_one, 0)
    part_two = jnp.einsum("cij,ia->jac", contracted, own_one, precision=HIGHEST).reshape(
        rows_two, rank * rank
    )
    slab_two = lax.psum_scatter(part_two, "row", scatter_dimension=1, tiled=True)
    slab_rows_two = lax.all_gather(slab_two, "col", axis=0, tiled=True)
    gram_two = lax.psum(right_product(slab_rows_two, slab_rows_two), "row")
    basis_two = settle(gram_two, lax.all_gather(start_two, "col", axis=0, tiled=True))
    own_two = lax.dynamic_slice_in_dim(basis_two, lax.axis_index("col") * rows_two, rows_two, 0)
    received = lax.all_to_all(tensor, "row", split_axis=2, concat_axis=0, tiled=True)
    count, items, cells = received.shape
    merged = left_product(basis_one, received.reshape(count, items * cells))
    mixed = merged.reshape(rank, items, cells)
    part_three = jnp.einsum("ajk,jb->kba", mixed, own_two, precision=HIGHEST)
    cells_here = part_three.shape[0]
    slab_three = lax.psum_scatter(
        part_three.reshape(cells_here, rank * rank), "col", scatter_dimension=1, tiled=True
    )
    gram_part_three = pairing(slab_three, lax.all_gather(slab_three, "row", axis=0, tiled=True))
    gram_three = lax.psum(gram_part_three, "col")
    basis_three = start_three
    own_three = start_three
    for iteration in range(STEPS):
        image = product(gram_three, basis_three)
        inner = lax.psum(left_product(image, image), "row")
        own_three = orthonormal(image, inner)
        basis_three = lax.all_gather(own_three, "row", axis=0, tiled=True)
    core_part = left_product(own_three, slab_three)
    core_part = core_part.reshape(rank, core_part.shape[1] // rank, rank)
    core = lax.psum_scatter(core_part, "row", scatter_dimension=2, tiled=True).transpose(0, 2, 1)
    factor_one = basis_one * math.sqrt(basis_one.shape[0])
    factor_two = basis_two * math.sqrt(basis_two.shape[0])
    factor_three = basis_three * math.sqrt(basis_three.shape[0])
    return (factor_one, factor_two, factor_three, core)


VMEM = pl.BlockSpec(memory_space=pltpu.VMEM)


def call(kernel, name, outs, *args, scratch=()):
    return pl.pallas_call(
        kernel,
        out_shape=[jax.ShapeDtypeStruct(shape, jnp.float32) for shape in outs],
        in_specs=[VMEM] * len(args),
        out_specs=[VMEM] * len(outs),
        scratch_shapes=[pltpu.VMEM(shape, jnp.float32) for shape in scratch],
        name=name,
    )(*args)


def iterate(gram, start):
    size = start.shape[0]
    extra = -size % WIDE
    gram = jnp.pad(gram, ((0, extra), (0, extra)))

    def step(_, turned):
        image = product(turned, gram)
        return product(lower_inverse(right_product(image, image)), image)

    return lax.fori_loop(0, STEPS, step, jnp.pad(start.T, ((0, 0), (0, extra))))[:, :size].T


def gram_of(slabs):
    total = right_product(slabs[0], slabs[0])
    for slab in slabs[1:]:
        total = total + right_product(slab, slab)
    return total


def open_kernel(cont_ref, start_ref, gram_ref):
    slabs = [product(cont_ref[c], start_ref[...]) for c in range(cont_ref.shape[0])]
    gram_ref[...] = gram_of(slabs)


def first_kernel(gram_ref, start_ref, cont_ref, basis_ref, factor_ref, next_ref):
    basis = iterate(gram_ref[...], start_ref[...])
    basis_ref[...] = basis
    factor_ref[...] = basis * math.sqrt(basis.shape[0])
    slabs = [left_product(cont_ref[c], basis) for c in range(cont_ref.shape[0])]
    next_ref[...] = gram_of(slabs)


def second_kernel(gram_ref, start_ref, factor_ref):
    basis = iterate(gram_ref[...], start_ref[...])
    factor_ref[...] = basis


def mix_kernel(factor_ref, cells_ref, mixed_ref, turn_ref, groups):
    ways, count, width = cells_ref.shape
    full, rank = factor_ref.shape
    span = BLOCK // groups
    lane = lax.broadcasted_iota(jnp.int32, (count, BLOCK), 1) // span
    tiles = width // BLOCK
    for r in range(ways // groups):
        for tile in range(tiles):
            held = [
                cells_ref[r * groups + c, :, tile * BLOCK : (tile + 1) * BLOCK] for c in range(groups)
            ]
            for inner in range(groups):
                piece = held[inner]
                for c in range(groups):
                    if c != inner:
                        moved = pltpu.roll(held[c], (c - inner) * span % BLOCK, 1)
                        piece = jnp.where(lane == c, moved, piece)
                index = (r * tiles + tile) * groups + inner
                turn_ref[pl.ds(index, count, stride=full), :] = piece
    for k in range(count):
        mixed_ref[k * rank : (k + 1) * rank] = left_product(
            factor_ref[...], turn_ref[k * full : (k + 1) * full]
        )


def slab_kernel(right_ref, mixed_ref, factor_ref, slab_ref, turn_ref, own_b):
    right = right_ref[...]
    factor_ref[...] = right * math.sqrt(right.shape[0])
    count, width = slab_ref.shape[1:]
    rank = right.shape[1]
    own_a, ways_two = width // own_b, rank // own_b
    turn_ref[...] = product(mixed_ref[...], jnp.pad(right, ((0, 0), (0, width - rank))))
    lane = lax.broadcasted_iota(jnp.int32, (count, width), 1) // own_b
    for r in range(rank // own_a):
        held = [turn_ref[pl.ds(r * own_a + a, count, stride=rank), :] for a in range(own_a)]
        for c in range(ways_two):
            piece = held[c % own_a]
            for a in range(own_a):
                if a != c:
                    moved = pltpu.roll(held[a], (a - c) * own_b % width, 1)
                    piece = jnp.where(lane == a, moved, piece)
            slab_ref[r * ways_two + c] = piece


def pairs(blocks):
    return [(i, j) for i in range(blocks) for j in range(i, blocks)]


def pair_kernel(slab_ref, gram_ref):
    row = 0
    for i in range(slab_ref.shape[0] // BLOCK):
        part = right_product(slab_ref[i * BLOCK :], slab_ref[i * BLOCK : (i + 1) * BLOCK])
        gram_ref[row : row + part.shape[0]] = part
        row += part.shape[0]


def third_kernel(packed_ref, start_ref, slab_ref, factor_ref, core_ref, gram_ref):
    for n, (i, j) in enumerate(pairs(slab_ref.shape[0] // BLOCK)):
        block = packed_ref[n * BLOCK : (n + 1) * BLOCK]
        gram_ref[j * BLOCK : (j + 1) * BLOCK, i * BLOCK : (i + 1) * BLOCK] = block
        if i != j:
            gram_ref[i * BLOCK : (i + 1) * BLOCK, j * BLOCK : (j + 1) * BLOCK] = block.T
    basis = iterate(gram_ref[...], start_ref[...])
    factor_ref[...] = basis * math.sqrt(basis.shape[0])
    core_ref[...] = left_product(basis, slab_ref[...])


def swap(x, axis, mask):
    count = lax.axis_size(axis)
    return lax.ppermute(x, axis, [(i, i ^ mask) for i in range(count)])


def tree(parts):
    while len(parts) > 1:
        parts = [parts[i] + parts[i + 1] for i in range(0, len(parts), 2)]
    return parts[0]


def sum_small(x):
    x = x + swap(x, "row", 1)
    x = tree([x] + [swap(x, "row", m) for m in range(2, lax.axis_size("row"), 2)])
    return tree([x] + [swap(x, "col", m) for m in range(1, lax.axis_size("col"))])


def bit(axis, mask):
    return (lax.axis_index(axis) & mask) != 0


def halve(x, axis, mask):
    rows = x.shape[0] // 2
    low, high = x[:rows], x[rows:]
    upper = bit(axis, mask)
    return jnp.where(upper, high, low) + swap(jnp.where(upper, low, high), axis, mask)


def double(x, axis, mask):
    other = swap(x, axis, mask)
    upper = bit(axis, mask)
    return jnp.concatenate([jnp.where(upper, other, x), jnp.where(upper, x, other)], axis=0)


def spread_rows(x, axis):
    count = lax.axis_size(axis)
    parts = [x] + [swap(x, axis, m) for m in range(1, count)]
    mask = 1
    while mask < count:
        upper = bit(axis, mask)
        parts = [jnp.where(upper, parts[i ^ mask], parts[i]) for i in range(count)]
        mask *= 2
    return jnp.concatenate(parts, axis=0)


def sum_large(x):
    x = halve(x, "row", 1)
    rows = x.shape[0] // 2
    masks = [m for m in (2, 4, 8, 16) if m < lax.axis_size("row")]
    lanes = [(x[:rows], masks), (x[rows:], masks[::-1])]
    done = []
    for part, order in lanes:
        for mask in order:
            part = halve(part, "row", mask)
        mask = 1
        while mask < lax.axis_size("col"):
            part = part + swap(part, "col", mask)
            mask *= 2
        for mask in order[::-1]:
            part = double(part, "row", mask)
        done.append(part)
    return double(jnp.concatenate(done, axis=0), "row", 1)


def swift(tensor, start_one, start_two, start_three):
    rows_one, rows_two, depth = tensor.shape
    rank = start_three.shape[1]
    ways_one, ways_two = lax.axis_size("row"), lax.axis_size("col")
    ways = ways_one * ways_two
    full_one, full_two = rows_one * ways_one, rows_two * ways_two
    flat = tensor.reshape(rows_one * rows_two, depth)
    two = spread_rows(start_two, "col")
    one = spread_rows(start_one, "row")

    def trade(x):
        shape = (ways, x.shape[0] // ways, x.shape[1])
        return lax.all_to_all(x.reshape(shape), AXES, 0, 0, tiled=True)

    contracted = trade(cross_product(start_three, flat))
    contracted = contracted.reshape(ways_one, ways_two, rank // ways, rows_one, rows_two)
    contracted = contracted.transpose(2, 0, 3, 1, 4).reshape(rank // ways, full_one, full_two)
    (gram,) = call(open_kernel, "open", [(full_one, full_one)], contracted, two)
    gram, one, turned = lax.optimization_barrier((sum_small(gram), one, flat.T))
    cells = trade(turned)
    basis_one, factor_one, gram = call(
        first_kernel,
        "first",
        [(full_one, rank), (full_one, rank), (full_two, full_two)],
        gram,
        one,
        contracted,
    )
    (basis_two,) = call(second_kernel, "second", [(full_two, rank)], sum_small(gram), two)
    count = depth // ways
    (mixed,) = call(
        functools.partial(mix_kernel, groups=ways_two),
        "mix",
        [(count * rank, full_two)],
        basis_one,
        cells,
        scratch=[(count * full_one, full_two)],
    )
    own_a, own_b = rank // ways_one, rank // ways_two
    factor_two, slab = call(
        functools.partial(slab_kernel, own_b=own_b),
        "slab",
        [(full_two, rank), (ways, count, own_a * own_b)],
        basis_two,
        mixed,
        scratch=[(count * rank, own_a * own_b)],
    )
    slab = lax.all_to_all(slab, AXES, 0, 0, tiled=True).reshape(depth, own_a * own_b)
    blocks = len(pairs(depth // BLOCK))
    (packed,) = call(pair_kernel, "pair", [(blocks * BLOCK, BLOCK)], slab)
    factor_three, core = pl.pallas_call(
        third_kernel,
        out_shape=[
            jax.ShapeDtypeStruct((depth, rank), jnp.float32),
            jax.ShapeDtypeStruct((rank, own_a * own_b), jnp.float32),
        ],
        in_specs=[VMEM] * 3,
        out_specs=[VMEM] * 2,
        scratch_shapes=[pltpu.VMEM((depth, depth), jnp.float32)],
        name="third",
    )(sum_large(packed), start_three, slab)
    return (factor_one, factor_two, factor_three, core.reshape(rank, own_a, own_b))


def power_of_two(value):
    return value & (value - 1) == 0


def on_device(tensor, start_one, start_two, start_three):
    rank, depth = start_three.shape[1], start_three.shape[0]
    ways_one, ways_two = lax.axis_size("row"), lax.axis_size("col")
    ways = ways_one * ways_two
    even = power_of_two(ways_one) and power_of_two(ways_two) and ways_one > 1
    blocks = len(pairs(depth // BLOCK)) * BLOCK
    even = even and tensor.shape[1] * ways_two == BLOCK and tensor.shape[0] % ways_two == 0
    even = even and rank * rank == BLOCK * ways and rank // ways_one >= ways_two
    even = even and rank % ways == 0 and depth % ways == 0 and depth % BLOCK == 0
    if even and blocks % (8 * 2 * ways_one) == 0:
        return swift(tensor, start_one, start_two, start_three)
    return general(tensor, start_one, start_two, start_three)


def solution(mesh):
    return jax.shard_map(
        on_device,
        mesh=mesh,
        in_specs=(P("row", "col", None), P("row", None), P("col", None), P()),
        out_specs=(P(), P(), P(), P(None, "row", "col")),
        check_vma=False,
    )
```

```python
import functools
import math

import jax
import jax.numpy as jnp
from jax import lax
from jax.experimental import pallas as pl
from jax.experimental.pallas import tpu as pltpu
from jax.sharding import PartitionSpec as P

STEPS = 4
PANEL = 8
BLOCK = 128
WIDE = 256
AXES = ("row", "col")

HIGHEST = lax.Precision.HIGHEST


def product(left, right):
    return jnp.dot(left, right, precision=HIGHEST, preferred_element_type=jnp.float32)


def left_product(left, right):
    return lax.dot_general(
        left, right, (((0,), (0,)), ((), ())), precision=HIGHEST, preferred_element_type=jnp.float32
    )


def right_product(left, right):
    return lax.dot_general(
        left, right, (((1,), (1,)), ((), ())), precision=HIGHEST, preferred_element_type=jnp.float32
    )


def cross_product(left, right):
    return lax.dot_general(
        left, right, (((0,), (1,)), ((), ())), precision=HIGHEST, preferred_element_type=jnp.float32
    )


def orthonormal(matrix, inner):
    lower = jnp.linalg.cholesky(inner)
    return jax.scipy.linalg.solve_triangular(lower, matrix.T, lower=True).T


def pairing(local, block_rows):
    return right_product(local, block_rows)


def spread(row, like):
    return jnp.broadcast_to(row, like.shape)


def lower_inverse(inner):
    size = inner.shape[0]
    eye = (
        lax.broadcasted_iota(jnp.int32, (size, size), 0) == lax.broadcasted_iota(jnp.int32, (size, size), 1)
    ).astype(jnp.float32)
    whole = jnp.concatenate([inner, eye], axis=1)
    panels = size // PANEL
    work = [whole[p * PANEL : (p + 1) * PANEL] for p in range(panels)]
    sub = lax.broadcasted_iota(jnp.int32, work[0].shape, 0)
    out = []
    for p in range(panels):
        cols = {
            i: [spread(work[i][:, p * PANEL + k : p * PANEL + k + 1], work[i]) for k in range(PANEL)]
            for i in range(p, panels)
        }
        scale = jnp.zeros_like(work[p])
        for k in range(PANEL):
            row = spread(work[p][k : k + 1], work[p])
            pivot = spread(cols[p][k][k : k + 1], work[p])
            scale = jnp.where(sub == k, lax.rsqrt(pivot), scale)
            recip = 1.0 / pivot
            across = [spread(cols[p][m][k : k + 1], work[p]) * recip for m in range(k + 1, PANEL)]
            row = row * recip
            for i in range(p, panels):
                factor = cols[i][k]
                if i == p:
                    factor = jnp.where(sub > k, factor, 0.0)
                work[i] = work[i] - factor * row
                for m in range(k + 1, PANEL):
                    cols[i][m] = cols[i][m] - factor * across[m - k - 1]
        out.append((work[p] * scale)[:, size:])
    return jnp.concatenate(out, axis=0)


def settle_kernel(gram_ref, start_ref, out_ref):
    out_ref[...] = iterate(gram_ref[...], start_ref[...].T).T


def settle(gram_whole, basis):
    return call(settle_kernel, "settle", [basis.shape], gram_whole, basis)[0]


def general(tensor, start_one, start_two, start_three):
    rows_one, rows_two, depth = tensor.shape
    rank = start_three.shape[1]
    flat = tensor.reshape(rows_one * rows_two, depth)
    contracted = cross_product(start_three, flat).reshape(rank, rows_one, rows_two)
    part_one = jnp.einsum("cij,jb->ibc", contracted, start_two, precision=HIGHEST).reshape(
        rows_one, rank * rank
    )
    slab_one = lax.psum_scatter(part_one, "col", scatter_dimension=1, tiled=True)
    slab_rows_one = lax.all_gather(slab_one, "row", axis=0, tiled=True)
    gram_one = lax.psum(right_product(slab_rows_one, slab_rows_one), "col")
    basis_one = settle(gram_one, lax.all_gather(start_one, "row", axis=0, tiled=True))
    own_one = lax.dynamic_slice_in_dim(basis_one, lax.axis_index("row") * rows_one, rows_one, 0)
    part_two = jnp.einsum("cij,ia->jac", contracted, own_one, precision=HIGHEST).reshape(
        rows_two, rank * rank
    )
    slab_two = lax.psum_scatter(part_two, "row", scatter_dimension=1, tiled=True)
    slab_rows_two = lax.all_gather(slab_two, "col", axis=0, tiled=True)
    gram_two = lax.psum(right_product(slab_rows_two, slab_rows_two), "row")
    basis_two = settle(gram_two, lax.all_gather(start_two, "col", axis=0, tiled=True))
    own_two = lax.dynamic_slice_in_dim(basis_two, lax.axis_index("col") * rows_two, rows_two, 0)
    received = lax.all_to_all(tensor, "row", split_axis=2, concat_axis=0, tiled=True)
    count, items, cells = received.shape
    merged = left_product(basis_one, received.reshape(count, items * cells))
    mixed = merged.reshape(rank, items, cells)
    part_three = jnp.einsum("ajk,jb->kba", mixed, own_two, precision=HIGHEST)
    cells_here = part_three.shape[0]
    slab_three = lax.psum_scatter(
        part_three.reshape(cells_here, rank * rank), "col", scatter_dimension=1, tiled=True
    )
    gram_part_three = pairing(slab_three, lax.all_gather(slab_three, "row", axis=0, tiled=True))
    gram_three = lax.psum(gram_part_three, "col")
    basis_three = start_three
    own_three = start_three
    for iteration in range(STEPS):
        image = product(gram_three, basis_three)
        inner = lax.psum(left_product(image, image), "row")
        own_three = orthonormal(image, inner)
        basis_three = lax.all_gather(own_three, "row", axis=0, tiled=True)
    core_part = left_product(own_three, slab_three)
    core_part = core_part.reshape(rank, core_part.shape[1] // rank, rank)
    core = lax.psum_scatter(core_part, "row", scatter_dimension=2, tiled=True).transpose(0, 2, 1)
    factor_one = basis_one * math.sqrt(basis_one.shape[0])
    factor_two = basis_two * math.sqrt(basis_two.shape[0])
    factor_three = basis_three * math.sqrt(basis_three.shape[0])
    return (factor_one, factor_two, factor_three, core)


VMEM = pl.BlockSpec(memory_space=pltpu.VMEM)


def call(kernel, name, outs, *args, scratch=()):
    return pl.pallas_call(
        kernel,
        out_shape=[jax.ShapeDtypeStruct(shape, jnp.float32) for shape in outs],
        in_specs=[VMEM] * len(args),
        out_specs=[VMEM] * len(outs),
        scratch_shapes=[pltpu.VMEM(shape, jnp.float32) for shape in scratch],
        name=name,
    )(*args)


def pieces(x):
    high = x.astype(jnp.bfloat16)
    rest = x - high.astype(jnp.float32)
    middle = rest.astype(jnp.bfloat16)
    low = (rest - middle.astype(jnp.float32)).astype(jnp.bfloat16)
    return high, middle, low


def iterate(gram, turned):
    rank, size = turned.shape
    extra = -size % WIDE
    high, middle, low = pieces(jnp.pad(gram, ((0, extra), (0, extra))))

    def times(parts, matrix):
        whole = jnp.dot(jnp.concatenate(parts, axis=0), matrix, preferred_element_type=jnp.float32)
        return [whole[n * rank : (n + 1) * rank] for n in range(len(parts))]

    def step(_, turned):
        top, mid, end = pieces(turned)
        first = times([top, mid, end], high)
        second = times([top, mid], middle)
        (third,) = times([top], low)
        image = first[0] + ((first[1] + second[0]) + ((first[2] + second[1]) + third))
        return product(lower_inverse(right_product(image, image)), image)

    return lax.fori_loop(0, STEPS, step, jnp.pad(turned, ((0, 0), (0, extra))))[:, :size]


def gram_of(slabs):
    total = right_product(slabs[0], slabs[0])
    for slab in slabs[1:]:
        total = total + right_product(slab, slab)
    return total


def open_kernel(cont_ref, start_ref, gram_ref):
    slabs = [product(cont_ref[c], start_ref[...]) for c in range(cont_ref.shape[0])]
    gram_ref[...] = gram_of(slabs)


def first_kernel(gram_ref, start_ref, cont_ref, basis_ref, factor_ref, next_ref):
    turned = iterate(gram_ref[...], start_ref[...].T)
    factor_ref[...] = turned * math.sqrt(turned.shape[1])
    basis = turned.T
    basis_ref[...] = basis
    slabs = [left_product(cont_ref[c], basis) for c in range(cont_ref.shape[0])]
    next_ref[...] = gram_of(slabs)


def second_kernel(gram_ref, start_ref, basis_ref, factor_ref):
    turned = iterate(gram_ref[...], start_ref[...].T)
    factor_ref[...] = turned * math.sqrt(turned.shape[1])
    basis_ref[...] = turned.T


def mix_kernel(factor_ref, cells_ref, mixed_ref, turn_ref, groups):
    ways, count, width = cells_ref.shape
    full, rank = factor_ref.shape
    span = BLOCK // groups
    lane = lax.broadcasted_iota(jnp.int32, (count, BLOCK), 1) // span
    tiles = width // BLOCK
    for r in range(ways // groups):
        for tile in range(tiles):
            held = [
                cells_ref[r * groups + c, :, tile * BLOCK : (tile + 1) * BLOCK] for c in range(groups)
            ]
            for inner in range(groups):
                piece = held[inner]
                for c in range(groups):
                    if c != inner:
                        moved = pltpu.roll(held[c], (c - inner) * span % BLOCK, 1)
                        piece = jnp.where(lane == c, moved, piece)
                index = (r * tiles + tile) * groups + inner
                turn_ref[pl.ds(index, count, stride=full), :] = piece
    for k in range(count):
        mixed_ref[k * rank : (k + 1) * rank] = left_product(
            factor_ref[...], turn_ref[k * full : (k + 1) * full]
        )


def slab_kernel(right_ref, mixed_ref, slab_ref, turn_ref, own_b):
    right = right_ref[...]
    count, width = slab_ref.shape[1:]
    rank = right.shape[1]
    own_a, ways_two = width // own_b, rank // own_b
    turn_ref[...] = product(mixed_ref[...], jnp.pad(right, ((0, 0), (0, width - rank))))
    lane = lax.broadcasted_iota(jnp.int32, (count, width), 1) // own_b
    for r in range(rank // own_a):
        held = [turn_ref[pl.ds(r * own_a + a, count, stride=rank), :] for a in range(own_a)]
        for c in range(ways_two):
            piece = held[c % own_a]
            for a in range(own_a):
                if a != c:
                    moved = pltpu.roll(held[a], (a - c) * own_b % width, 1)
                    piece = jnp.where(lane == a, moved, piece)
            slab_ref[r * ways_two + c] = piece


def pairs(blocks):
    return [(i, j) for i in range(blocks) for j in range(i, blocks)]


def pair_kernel(slab_ref, gram_ref):
    row = 0
    for i in range(slab_ref.shape[0] // BLOCK):
        part = right_product(slab_ref[i * BLOCK :], slab_ref[i * BLOCK : (i + 1) * BLOCK])
        gram_ref[row : row + part.shape[0]] = part
        row += part.shape[0]


def third_kernel(packed_ref, start_ref, slab_ref, factor_ref, core_ref, gram_ref):
    for n, (i, j) in enumerate(pairs(slab_ref.shape[0] // BLOCK)):
        block = packed_ref[n * BLOCK : (n + 1) * BLOCK]
        gram_ref[j * BLOCK : (j + 1) * BLOCK, i * BLOCK : (i + 1) * BLOCK] = block
        if i != j:
            gram_ref[i * BLOCK : (i + 1) * BLOCK, j * BLOCK : (j + 1) * BLOCK] = block.T
    turned = iterate(gram_ref[...], start_ref[...])
    factor_ref[...] = turned * math.sqrt(turned.shape[1])
    core_ref[...] = product(turned, slab_ref[...]).T


def swap(x, axis, mask):
    count = lax.axis_size(axis)
    return lax.ppermute(x, axis, [(i, i ^ mask) for i in range(count)])


def tree(parts):
    while len(parts) > 1:
        parts = [parts[i] + parts[i + 1] for i in range(0, len(parts), 2)]
    return parts[0]


def sum_small(x):
    x = x + swap(x, "row", 1)
    x = tree([x] + [swap(x, "row", m) for m in range(2, lax.axis_size("row"), 2)])
    return tree([x] + [swap(x, "col", m) for m in range(1, lax.axis_size("col"))])


def bit(axis, mask):
    return (lax.axis_index(axis) & mask) != 0


def halve(x, axis, mask):
    rows = x.shape[0] // 2
    low, high = x[:rows], x[rows:]
    upper = bit(axis, mask)
    return jnp.where(upper, high, low) + swap(jnp.where(upper, low, high), axis, mask)


def double(x, axis, mask):
    other = swap(x, axis, mask)
    upper = bit(axis, mask)
    return jnp.concatenate([jnp.where(upper, other, x), jnp.where(upper, x, other)], axis=0)


def spread_rows(x, axis):
    count = lax.axis_size(axis)
    parts = [x] + [swap(x, axis, m) for m in range(1, count)]
    mask = 1
    while mask < count:
        upper = bit(axis, mask)
        parts = [jnp.where(upper, parts[i ^ mask], parts[i]) for i in range(count)]
        mask *= 2
    return jnp.concatenate(parts, axis=0)


def gather_rows(x, axis):
    mask = 1
    while mask < lax.axis_size(axis):
        x = double(x, axis, mask)
        mask *= 2
    return x


def sum_large(x):
    x = halve(x, "row", 1)
    rows = x.shape[0] // 2
    masks = [m for m in (2, 4, 8, 16) if m < lax.axis_size("row")]
    lanes = [(x[:rows], masks), (x[rows:], masks[::-1])]
    done = []
    for part, order in lanes:
        for mask in order:
            part = halve(part, "row", mask)
        mask = 1
        while mask < lax.axis_size("col"):
            part = part + swap(part, "col", mask)
            mask *= 2
        for mask in order[::-1]:
            part = double(part, "row", mask)
        done.append(part)
    return double(jnp.concatenate(done, axis=0), "row", 1)


def swift(tensor, start_one, start_two, start_three):
    rows_one, rows_two, depth = tensor.shape
    rank = start_three.shape[1]
    ways_one, ways_two = lax.axis_size("row"), lax.axis_size("col")
    ways = ways_one * ways_two
    full_one, full_two = rows_one * ways_one, rows_two * ways_two
    flat = tensor.reshape(rows_one * rows_two, depth)

    def trade(x):
        shape = (ways, x.shape[0] // ways, x.shape[1])
        return lax.all_to_all(x.reshape(shape), AXES, 0, 0, tiled=True)

    local = cross_product(start_three, flat)
    local, start_one, start_two = lax.optimization_barrier((local, start_one, start_two))
    two = spread_rows(start_two, "col")
    one = gather_rows(start_one, "row")
    contracted = trade(local)
    contracted = contracted.reshape(ways_one, ways_two, rank // ways, rows_one, rows_two)
    contracted = contracted.transpose(2, 0, 3, 1, 4).reshape(rank // ways, full_one, full_two)
    (gram,) = call(open_kernel, "open", [(full_one, full_one)], contracted, two)
    gram, one, turned = lax.optimization_barrier((sum_small(gram), one, flat.T))
    cells = trade(turned)
    basis_one, factor_one, gram = call(
        first_kernel,
        "first",
        [(full_one, rank), (rank, full_one), (full_two, full_two)],
        gram,
        one,
        contracted,
    )
    basis_two, factor_two = call(
        second_kernel, "second", [(full_two, rank), (rank, full_two)], sum_small(gram), two
    )
    count = depth // ways
    (mixed,) = call(
        functools.partial(mix_kernel, groups=ways_two),
        "mix",
        [(count * rank, full_two)],
        basis_one,
        cells,
        scratch=[(count * full_one, full_two)],
    )
    own_a, own_b = rank // ways_one, rank // ways_two
    (slab,) = call(
        functools.partial(slab_kernel, own_b=own_b),
        "slab",
        [(ways, count, own_a * own_b)],
        basis_two,
        mixed,
        scratch=[(count * rank, own_a * own_b)],
    )
    slab = lax.all_to_all(slab, AXES, 0, 0, tiled=True).reshape(depth, own_a * own_b)
    blocks = len(pairs(depth // BLOCK))
    (packed,) = call(pair_kernel, "pair", [(blocks * BLOCK, BLOCK)], slab)
    factor_three, core = pl.pallas_call(
        third_kernel,
        out_shape=[
            jax.ShapeDtypeStruct((rank, depth), jnp.float32),
            jax.ShapeDtypeStruct((own_a * own_b, rank), jnp.float32),
        ],
        in_specs=[VMEM] * 3,
        out_specs=[VMEM] * 2,
        scratch_shapes=[pltpu.VMEM((depth, depth), jnp.float32)],
        name="third",
    )(sum_large(packed), start_three.T, slab)
    return (factor_one.T, factor_two.T, factor_three.T, core.T.reshape(rank, own_a, own_b))


def power_of_two(value):
    return value & (value - 1) == 0


def on_device(tensor, start_one, start_two, start_three):
    rank, depth = start_three.shape[1], start_three.shape[0]
    ways_one, ways_two = lax.axis_size("row"), lax.axis_size("col")
    ways = ways_one * ways_two
    even = power_of_two(ways_one) and power_of_two(ways_two) and ways_one > 1
    blocks = len(pairs(depth // BLOCK)) * BLOCK
    even = even and tensor.shape[1] * ways_two == BLOCK and tensor.shape[0] % ways_two == 0
    even = even and rank * rank == BLOCK * ways and rank // ways_one >= ways_two
    even = even and rank % ways == 0 and depth % ways == 0 and depth % BLOCK == 0
    if even and blocks % (8 * 2 * ways_one) == 0:
        return swift(tensor, start_one, start_two, start_three)
    return general(tensor, start_one, start_two, start_three)


def solution(mesh):
    return jax.shard_map(
        on_device,
        mesh=mesh,
        in_specs=(P("row", "col", None), P("row", None), P("col", None), P()),
        out_specs=(P(), P(), P(), P(None, "row", "col")),
        check_vma=False,
    )
```

```python
import functools
import math

import jax
import jax.numpy as jnp
from jax import lax
from jax.experimental import pallas as pl
from jax.experimental.pallas import tpu as pltpu
from jax.sharding import PartitionSpec as P

STEPS = 4
PANEL = 8
BLOCK = 128
WIDE = 256
AXES = ("row", "col")

HIGHEST = lax.Precision.HIGHEST


def product(left, right):
    return jnp.dot(left, right, precision=HIGHEST, preferred_element_type=jnp.float32)


def left_product(left, right):
    return lax.dot_general(
        left, right, (((0,), (0,)), ((), ())), precision=HIGHEST, preferred_element_type=jnp.float32
    )


def right_product(left, right):
    return lax.dot_general(
        left, right, (((1,), (1,)), ((), ())), precision=HIGHEST, preferred_element_type=jnp.float32
    )


def cross_product(left, right):
    return lax.dot_general(
        left, right, (((0,), (1,)), ((), ())), precision=HIGHEST, preferred_element_type=jnp.float32
    )


def orthonormal(matrix, inner):
    lower = jnp.linalg.cholesky(inner)
    return jax.scipy.linalg.solve_triangular(lower, matrix.T, lower=True).T


def pairing(local, block_rows):
    return right_product(local, block_rows)


def spread(row, like):
    return jnp.broadcast_to(row, like.shape)


def lower_inverse(inner):
    size = inner.shape[0]
    eye = (
        lax.broadcasted_iota(jnp.int32, (size, size), 0) == lax.broadcasted_iota(jnp.int32, (size, size), 1)
    ).astype(jnp.float32)
    whole = jnp.concatenate([inner, eye], axis=1)
    panels = size // PANEL
    work = [whole[p * PANEL : (p + 1) * PANEL] for p in range(panels)]
    sub = lax.broadcasted_iota(jnp.int32, work[0].shape, 0)
    out = []
    for p in range(panels):
        cols = {
            i: [spread(work[i][:, p * PANEL + k : p * PANEL + k + 1], work[i]) for k in range(PANEL)]
            for i in range(p, panels)
        }
        scale = jnp.zeros_like(work[p])
        for k in range(PANEL):
            row = spread(work[p][k : k + 1], work[p])
            pivot = spread(cols[p][k][k : k + 1], work[p])
            scale = jnp.where(sub == k, lax.rsqrt(pivot), scale)
            recip = 1.0 / pivot
            across = [spread(cols[p][m][k : k + 1], work[p]) * recip for m in range(k + 1, PANEL)]
            row = row * recip
            for i in range(p, panels):
                factor = cols[i][k]
                if i == p:
                    factor = jnp.where(sub > k, factor, 0.0)
                work[i] = work[i] - factor * row
                for m in range(k + 1, PANEL):
                    cols[i][m] = cols[i][m] - factor * across[m - k - 1]
        out.append((work[p] * scale)[:, size:])
    return jnp.concatenate(out, axis=0)


def settle_kernel(gram_ref, start_ref, out_ref):
    out_ref[...] = iterate(gram_ref[...], start_ref[...].T).T


def settle(gram_whole, basis):
    return call(settle_kernel, "settle", [basis.shape], gram_whole, basis)[0]


def general(tensor, start_one, start_two, start_three):
    rows_one, rows_two, depth = tensor.shape
    rank = start_three.shape[1]
    flat = tensor.reshape(rows_one * rows_two, depth)
    contracted = cross_product(start_three, flat).reshape(rank, rows_one, rows_two)
    part_one = jnp.einsum("cij,jb->ibc", contracted, start_two, precision=HIGHEST).reshape(
        rows_one, rank * rank
    )
    slab_one = lax.psum_scatter(part_one, "col", scatter_dimension=1, tiled=True)
    slab_rows_one = lax.all_gather(slab_one, "row", axis=0, tiled=True)
    gram_one = lax.psum(right_product(slab_rows_one, slab_rows_one), "col")
    basis_one = settle(gram_one, lax.all_gather(start_one, "row", axis=0, tiled=True))
    own_one = lax.dynamic_slice_in_dim(basis_one, lax.axis_index("row") * rows_one, rows_one, 0)
    part_two = jnp.einsum("cij,ia->jac", contracted, own_one, precision=HIGHEST).reshape(
        rows_two, rank * rank
    )
    slab_two = lax.psum_scatter(part_two, "row", scatter_dimension=1, tiled=True)
    slab_rows_two = lax.all_gather(slab_two, "col", axis=0, tiled=True)
    gram_two = lax.psum(right_product(slab_rows_two, slab_rows_two), "row")
    basis_two = settle(gram_two, lax.all_gather(start_two, "col", axis=0, tiled=True))
    own_two = lax.dynamic_slice_in_dim(basis_two, lax.axis_index("col") * rows_two, rows_two, 0)
    received = lax.all_to_all(tensor, "row", split_axis=2, concat_axis=0, tiled=True)
    count, items, cells = received.shape
    merged = left_product(basis_one, received.reshape(count, items * cells))
    mixed = merged.reshape(rank, items, cells)
    part_three = jnp.einsum("ajk,jb->kba", mixed, own_two, precision=HIGHEST)
    cells_here = part_three.shape[0]
    slab_three = lax.psum_scatter(
        part_three.reshape(cells_here, rank * rank), "col", scatter_dimension=1, tiled=True
    )
    gram_part_three = pairing(slab_three, lax.all_gather(slab_three, "row", axis=0, tiled=True))
    gram_three = lax.psum(gram_part_three, "col")
    basis_three = start_three
    own_three = start_three
    for iteration in range(STEPS):
        image = product(gram_three, basis_three)
        inner = lax.psum(left_product(image, image), "row")
        own_three = orthonormal(image, inner)
        basis_three = lax.all_gather(own_three, "row", axis=0, tiled=True)
    core_part = left_product(own_three, slab_three)
    core_part = core_part.reshape(rank, core_part.shape[1] // rank, rank)
    core = lax.psum_scatter(core_part, "row", scatter_dimension=2, tiled=True).transpose(0, 2, 1)
    factor_one = basis_one * math.sqrt(basis_one.shape[0])
    factor_two = basis_two * math.sqrt(basis_two.shape[0])
    factor_three = basis_three * math.sqrt(basis_three.shape[0])
    return (factor_one, factor_two, factor_three, core)


VMEM = pl.BlockSpec(memory_space=pltpu.VMEM)


def call(kernel, name, outs, *args, scratch=()):
    return pl.pallas_call(
        kernel,
        out_shape=[jax.ShapeDtypeStruct(shape, jnp.float32) for shape in outs],
        in_specs=[VMEM] * len(args),
        out_specs=[VMEM] * len(outs),
        scratch_shapes=[pltpu.VMEM(shape, jnp.float32) for shape in scratch],
        name=name,
    )(*args)


def pieces(x):
    high = x.astype(jnp.bfloat16)
    rest = x - high.astype(jnp.float32)
    middle = rest.astype(jnp.bfloat16)
    low = (rest - middle.astype(jnp.float32)).astype(jnp.bfloat16)
    return high, middle, low


def stacked(left, right):
    rows = left[0].shape[0]

    def times(parts, matrix):
        whole = jnp.dot(jnp.concatenate(parts, axis=0), matrix, preferred_element_type=jnp.float32)
        return [whole[n * rows : (n + 1) * rows] for n in range(len(parts))]

    first = times(left, right[0])
    second = times(left[:2], right[1])
    (third,) = times(left[:1], right[2])
    return first[0] + ((first[1] + second[0]) + ((first[2] + second[1]) + third))


def iterate(gram, turned):
    extra = -turned.shape[1] % WIDE
    parts = pieces(jnp.pad(gram, ((0, extra), (0, extra))))

    def step(_, turned):
        image = stacked(pieces(turned), parts)
        return product(lower_inverse(right_product(image, image)), image)

    size = turned.shape[1]
    return lax.fori_loop(0, STEPS, step, jnp.pad(turned, ((0, 0), (0, extra))))[:, :size]


def gram_of(slabs):
    total = right_product(slabs[0], slabs[0])
    for slab in slabs[1:]:
        total = total + right_product(slab, slab)
    return total


def open_kernel(cont_ref, start_ref, gram_ref):
    slabs = [product(cont_ref[c], start_ref[...]) for c in range(cont_ref.shape[0])]
    gram_ref[...] = gram_of(slabs)


def first_kernel(*refs):
    start_ref, cont_ref, basis_ref, factor_ref, next_ref = refs[-5:]
    turned = iterate(tree([ref[...] for ref in refs[:-5]]), start_ref[...].T)
    factor_ref[...] = turned * math.sqrt(turned.shape[1])
    basis = turned.T
    basis_ref[...] = basis
    slabs = [left_product(cont_ref[c], basis) for c in range(cont_ref.shape[0])]
    next_ref[...] = gram_of(slabs)


def second_kernel(*refs):
    start_ref, basis_ref, factor_ref = refs[-3:]
    turned = iterate(tree([ref[...] for ref in refs[:-3]]), start_ref[...].T)
    factor_ref[...] = turned * math.sqrt(turned.shape[1])
    basis_ref[...] = turned.T


def mix_kernel(factor_ref, cells_ref, mixed_ref, turn_ref, groups):
    ways, count, width = cells_ref.shape
    full, rank = factor_ref.shape
    span = BLOCK // groups
    lane = lax.broadcasted_iota(jnp.int32, (count, BLOCK), 1) // span
    tiles = width // BLOCK
    for r in range(ways // groups):
        for tile in range(tiles):
            held = [
                cells_ref[r * groups + c, :, tile * BLOCK : (tile + 1) * BLOCK] for c in range(groups)
            ]
            for inner in range(groups):
                piece = held[inner]
                for c in range(groups):
                    if c != inner:
                        moved = pltpu.roll(held[c], (c - inner) * span % BLOCK, 1)
                        piece = jnp.where(lane == c, moved, piece)
                index = (r * tiles + tile) * groups + inner
                turn_ref[pl.ds(index, count, stride=full), :] = piece
    parts = pieces(factor_ref[...].T)
    for k in range(count):
        mixed_ref[k * rank : (k + 1) * rank] = stacked(parts, pieces(turn_ref[k * full : (k + 1) * full]))


def slab_kernel(right_ref, mixed_ref, slab_ref, turn_ref, own_b):
    right = right_ref[...]
    count, width = slab_ref.shape[1:]
    rank = right.shape[1]
    own_a, ways_two = width // own_b, rank // own_b
    turn_ref[...] = product(mixed_ref[...], jnp.pad(right, ((0, 0), (0, width - rank))))
    lane = lax.broadcasted_iota(jnp.int32, (count, width), 1) // own_b
    for r in range(rank // own_a):
        held = [turn_ref[pl.ds(r * own_a + a, count, stride=rank), :] for a in range(own_a)]
        for c in range(ways_two):
            piece = held[c % own_a]
            for a in range(own_a):
                if a != c:
                    moved = pltpu.roll(held[a], (a - c) * own_b % width, 1)
                    piece = jnp.where(lane == a, moved, piece)
            slab_ref[r * ways_two + c] = piece


def pairs(blocks):
    return [(i, j) for i in range(blocks) for j in range(i, blocks)]


def pair_kernel(slab_ref, gram_ref):
    row = 0
    for i in range(slab_ref.shape[0] // BLOCK):
        part = right_product(slab_ref[i * BLOCK :], slab_ref[i * BLOCK : (i + 1) * BLOCK])
        gram_ref[row : row + part.shape[0]] = part
        row += part.shape[0]


def third_kernel(packed_ref, start_ref, slab_ref, factor_ref, core_ref, gram_ref):
    for n, (i, j) in enumerate(pairs(slab_ref.shape[0] // BLOCK)):
        block = packed_ref[n * BLOCK : (n + 1) * BLOCK]
        gram_ref[j * BLOCK : (j + 1) * BLOCK, i * BLOCK : (i + 1) * BLOCK] = block
        if i != j:
            gram_ref[i * BLOCK : (i + 1) * BLOCK, j * BLOCK : (j + 1) * BLOCK] = block.T
    turned = iterate(gram_ref[...], start_ref[...])
    factor_ref[...] = turned * math.sqrt(turned.shape[1])
    core_ref[...] = product(turned, slab_ref[...]).T


def swap(x, axis, mask):
    count = lax.axis_size(axis)
    return lax.ppermute(x, axis, [(i, i ^ mask) for i in range(count)])


def tree(parts):
    while len(parts) > 1:
        parts = [parts[i] + parts[i + 1] for i in range(0, len(parts), 2)]
    return parts[0]


def sum_small(x):
    x = x + swap(x, "row", 1)
    x = tree([x] + [swap(x, "row", m) for m in range(2, lax.axis_size("row"), 2)])
    return [x] + [swap(x, "col", m) for m in range(1, lax.axis_size("col"))]


def bit(axis, mask):
    return (lax.axis_index(axis) & mask) != 0


def halve(x, axis, mask):
    rows = x.shape[0] // 2
    low, high = x[:rows], x[rows:]
    upper = bit(axis, mask)
    return jnp.where(upper, high, low) + swap(jnp.where(upper, low, high), axis, mask)


def double(x, axis, mask):
    other = swap(x, axis, mask)
    upper = bit(axis, mask)
    return jnp.concatenate([jnp.where(upper, other, x), jnp.where(upper, x, other)], axis=0)


def spread_rows(x, axis):
    count = lax.axis_size(axis)
    parts = [x] + [swap(x, axis, m) for m in range(1, count)]
    mask = 1
    while mask < count:
        upper = bit(axis, mask)
        parts = [jnp.where(upper, parts[i ^ mask], parts[i]) for i in range(count)]
        mask *= 2
    return jnp.concatenate(parts, axis=0)


def gather_rows(x, axis):
    mask = 1
    while mask < lax.axis_size(axis):
        x = double(x, axis, mask)
        mask *= 2
    return x


def sum_large(x):
    x = halve(x, "row", 1)
    rows = x.shape[0] // 2
    masks = [m for m in (2, 4, 8, 16) if m < lax.axis_size("row")]
    lanes = [(x[:rows], masks), (x[rows:], masks[::-1])]
    done = []
    for part, order in lanes:
        for mask in order:
            part = halve(part, "row", mask)
        mask = 1
        while mask < lax.axis_size("col"):
            part = part + swap(part, "col", mask)
            mask *= 2
        for mask in order[::-1]:
            part = double(part, "row", mask)
        done.append(part)
    return double(jnp.concatenate(done, axis=0), "row", 1)


def swift(tensor, start_one, start_two, start_three):
    rows_one, rows_two, depth = tensor.shape
    rank = start_three.shape[1]
    ways_one, ways_two = lax.axis_size("row"), lax.axis_size("col")
    ways = ways_one * ways_two
    full_one, full_two = rows_one * ways_one, rows_two * ways_two
    flat = tensor.reshape(rows_one * rows_two, depth)

    def trade(x):
        shape = (ways, x.shape[0] // ways, x.shape[1])
        return lax.all_to_all(x.reshape(shape), AXES, 0, 0, tiled=True)

    local = cross_product(start_three, flat)
    local, start_one, start_two = lax.optimization_barrier((local, start_one, start_two))
    two = spread_rows(start_two, "col")
    one = gather_rows(start_one, "row")
    contracted = trade(local)
    contracted = contracted.reshape(ways_one, ways_two, rank // ways, rows_one, rows_two)
    contracted = contracted.transpose(2, 0, 3, 1, 4).reshape(rank // ways, full_one, full_two)
    (gram,) = call(open_kernel, "open", [(full_one, full_one)], contracted, two)
    gram, one, turned = lax.optimization_barrier((sum_small(gram), one, flat.T))
    cells = trade(turned)
    basis_one, factor_one, gram = call(
        first_kernel,
        "first",
        [(full_one, rank), (rank, full_one), (full_two, full_two)],
        *gram,
        one,
        contracted,
    )
    basis_two, factor_two = call(
        second_kernel, "second", [(full_two, rank), (rank, full_two)], *sum_small(gram), two
    )
    count = depth // ways
    (mixed,) = call(
        functools.partial(mix_kernel, groups=ways_two),
        "mix",
        [(count * rank, full_two)],
        basis_one,
        cells,
        scratch=[(count * full_one, full_two)],
    )
    own_a, own_b = rank // ways_one, rank // ways_two
    (slab,) = call(
        functools.partial(slab_kernel, own_b=own_b),
        "slab",
        [(ways, count, own_a * own_b)],
        basis_two,
        mixed,
        scratch=[(count * rank, own_a * own_b)],
    )
    slab = lax.all_to_all(slab, AXES, 0, 0, tiled=True).reshape(depth, own_a * own_b)
    blocks = len(pairs(depth // BLOCK))
    (packed,) = call(pair_kernel, "pair", [(blocks * BLOCK, BLOCK)], slab)
    factor_three, core = pl.pallas_call(
        third_kernel,
        out_shape=[
            jax.ShapeDtypeStruct((rank, depth), jnp.float32),
            jax.ShapeDtypeStruct((own_a * own_b, rank), jnp.float32),
        ],
        in_specs=[VMEM] * 3,
        out_specs=[VMEM] * 2,
        scratch_shapes=[pltpu.VMEM((depth, depth), jnp.float32)],
        name="third",
    )(sum_large(packed), start_three.T, slab)
    return (factor_one.T, factor_two.T, factor_three.T, core.T.reshape(rank, own_a, own_b))


def power_of_two(value):
    return value & (value - 1) == 0


def on_device(tensor, start_one, start_two, start_three):
    rank, depth = start_three.shape[1], start_three.shape[0]
    ways_one, ways_two = lax.axis_size("row"), lax.axis_size("col")
    ways = ways_one * ways_two
    even = power_of_two(ways_one) and power_of_two(ways_two) and ways_one > 1
    blocks = len(pairs(depth // BLOCK)) * BLOCK
    even = even and tensor.shape[1] * ways_two == BLOCK and tensor.shape[0] % ways_two == 0
    even = even and rank * rank == BLOCK * ways and rank // ways_one >= ways_two
    even = even and rank % ways == 0 and depth % ways == 0 and depth % BLOCK == 0
    if even and blocks % (8 * 2 * ways_one) == 0:
        return swift(tensor, start_one, start_two, start_three)
    return general(tensor, start_one, start_two, start_three)


def solution(mesh):
    return jax.shard_map(
        on_device,
        mesh=mesh,
        in_specs=(P("row", "col", None), P("row", None), P("col", None), P()),
        out_specs=(P(), P(), P(), P(None, "row", "col")),
        check_vma=False,
    )
```
